32 devices in a mesh: vocab: 8 (over z, y), dp: 4 (over x, core).
Axes of the slice: x: 2, y: 2, z: 4, core: 2. Of those that a mesh axis runs over, the one named last changes fastest.
Arguments:
- hidden: bfloat16 [4096, 4096], P('dp'), may hold values from -6 to 6
- labels: int32 [4096], P('dp'), may hold values from 0 to 3, as said below
- targets: int32 [4096], P('dp'), may hold values from 0 to 147455, as said below
- head_weight: bfloat16 [4096, 16384], P(None, 'vocab'), may hold values from -0.125 to 0.125
- cluster_weight: bfloat16 [4096, 3], replicated, may hold values from -0.09375 to 0.09375
- proj_one: bfloat16 [4096, 1024], P('vocab'), may hold values from -0.09375 to 0.09375
- proj_two: bfloat16 [4096, 256], P('vocab'), may hold values from -0.09375 to 0.09375
- proj_three: bfloat16 [4096, 64], P('vocab'), may hold values from -0.09375 to 0.09375
- out_one: bfloat16 [1024, 32768], P(None, 'vocab'), may hold values from -0.1875 to 0.1875
- out_two: bfloat16 [256, 65536], P(None, 'vocab'), may hold values from -0.375 to 0.375
- out_three: bfloat16 [64, 147456], P(None, 'vocab'), may hold values from -0.75 to 0.75
Outputs:
- token_loss: float32 [4096], P('dp')
- mean_loss: float32 [], replicated
- hidden_grad: float32 [4096, 4096], P('dp', 'vocab')
The draws below stay inside these ranges and needn't reach their ends.
Inputs may be any that keep to these rules, and one draw needn't show every extreme that they name: In each aligned block of 1024 tokens (one index of dp), each of the labels 1, 2 and 3 marks at most 256 tokens and at least 128; for each label some block holds exactly 256 of them. `targets`: A token's target is below 16384 if its label is 0, below 32768, 65536 or 147456 if its label is 1, 2 or 3.
All inputs are finite; a program needn't handle non-finite values.
Results may differ from the reference program's by a relative error of at most 0.0013.
Values sent between devices are 32-bit elements; how exact they have to be, the bound alone decides.
No kernel may reach another device: no remote copies, remote signals or barrier semaphores. Data moves between devices by JAX's collectives and lax.ppermute only.
A program may use at most 128 MiB of HBM per device.

```python
import jax
import jax.numpy as jnp
from jax import lax

D = 4096
HEAD = 16384
P1 = 1024
P2 = 256
P3 = 64
V1 = 32768
V2 = 65536
V3 = 147456
GRP_TOK = 1024
CAP = 256
TOKENS = 4096


def label_parts(key):
    groups = TOKENS // GRP_TOK
    first_key, second_key, third_key, fourth_key = jax.random.split(jax.random.fold_in(key, 17), 4)
    full_group = jax.random.randint(first_key, (3,), 0, groups)
    amounts = jax.random.randint(second_key, (groups, 3), CAP // 2, CAP + 1)
    amounts = jnp.where(jnp.arange(groups)[:, None] == full_group[None, :], CAP, amounts).astype(jnp.int32)
    edges = jnp.cumsum(amounts, axis=1)
    places = jnp.arange(GRP_TOK, dtype=jnp.int32)[None, :]
    sorted_labels = jnp.where(places < edges[:, 0:1], 1, jnp.where(places < edges[:, 1:2], 2, jnp.where(places < edges[:, 2:3], 3, 0)))
    shuffles = jax.vmap(lambda sub_key: jax.random.permutation(sub_key, GRP_TOK))(jax.random.split(third_key, groups))
    labels = jnp.take_along_axis(sorted_labels, shuffles, axis=1).reshape(TOKENS).astype(jnp.int32)
    limits = jnp.array([HEAD, V1, V2, V3], jnp.int32)[labels]
    raw_ids = jax.random.randint(fourth_key, (TOKENS,), 0, 2 ** 30, dtype=jnp.int32)
    targets = (raw_ids % limits).astype(jnp.int32)
    return (labels, targets)


def draw_labels(key, part):
    return label_parts(key)[0]


def draw_targets(key, part):
    return label_parts(key)[1]


def raised(values, own_key, source, target, shards_of, factor):
    owner, partner = [(jnp.arange(values.shape[axis_at]) // (values.shape[axis_at] // shards_of)).reshape([-1 if axis == axis_at else 1 for axis in range(values.ndim)]) for axis_at in (source, target)]
    chosen = jax.random.permutation(own_key, shards_of)[partner]
    strong = (owner == chosen) | (owner == (partner + shards_of // 2) % shards_of)
    return jnp.where(strong, factor * values, values)


def levels(key, extent, pieces, smallest, largest):
    loudness = 1.0
    for position, shards_of in pieces:
        steps = jax.random.uniform(jax.random.fold_in(jax.random.fold_in(key, 6), position), (shards_of,), jnp.float32, smallest / len(pieces), largest / len(pieces))
        loudness = loudness * jnp.repeat(jnp.exp(steps), extent[position] // shards_of).reshape((-1,) + (1,) * (len(extent) - 1 - position))
    return loudness


def gaussian(key, extent, deviation, most, cuts=(), kind=jnp.bfloat16):
    factor_of = levels(key, extent, cuts, -0.22, 0.18) if cuts else 1.0
    values = jax.random.normal(key, extent, jnp.float32) * deviation * factor_of
    return jnp.minimum(jnp.maximum(values, -most), most).astype(kind)


def bell_draw_with(key, extent, width, reach, shards, heavy, kind=jnp.bfloat16):
    values = width * jax.random.normal(key, extent, jnp.float32)
    if shards:
        values = values * levels(key, extent, shards, -0.22, 0.18)
    return jnp.clip(raised(values, jax.random.fold_in(key, 3), *heavy), -reach, reach).astype(kind)


def setup_inputs(seed: int = 0) -> dict:
    streams_of = jax.random.split(jax.random.key(seed), 12)
    hidden = gaussian(streams_of[0], (TOKENS, D), 1.0, 6.0, ((0, 4),))
    labels = draw_labels(jax.random.fold_in(streams_of[11], 71), 0)
    targets = draw_targets(jax.random.fold_in(streams_of[11], 71), 0)
    head_weight = bell_draw_with(streams_of[3], (D, HEAD), D ** -0.5, 0.125, ((1, 8),), (1, 0, 8, 2.0))
    cluster_weight = gaussian(streams_of[4], (D, 3), D ** -0.5, 0.09375)
    proj_one = gaussian(streams_of[5], (D, P1), D ** -0.5, 0.09375, ((0, 8),))
    proj_two = gaussian(streams_of[6], (D, P2), D ** -0.5, 0.09375, ((0, 8),))
    proj_three = gaussian(streams_of[7], (D, P3), D ** -0.5, 0.09375, ((0, 8),))
    out_one = gaussian(streams_of[8], (P1, V1), P1 ** -0.5, 0.1875, ((1, 8),))
    out_two = gaussian(streams_of[9], (P2, V2), P2 ** -0.5, 0.375, ((1, 8),))
    out_three = gaussian(streams_of[10], (P3, V3), P3 ** -0.5, 0.75, ((1, 8),))
    return {"hidden": hidden, "labels": labels, "targets": targets, "head_weight": head_weight, "cluster_weight": cluster_weight, "proj_one": proj_one, "proj_two": proj_two, "proj_three": proj_three, "out_one": out_one, "out_two": out_two, "out_three": out_three}


capping = 30.0

def capped(values):
    return capping * jnp.tanh(values / capping)

def cluster_slots(labels, cluster, capacity):
    member = labels == cluster
    placed = jnp.cumsum(member.astype(jnp.int32)) - 1
    slot_of = jnp.where(member, placed, capacity).astype(jnp.int32)
    order = jnp.arange(labels.shape[0], dtype=jnp.int32)
    slot_rows = jnp.zeros((capacity + 1,), jnp.int32).at[slot_of].set(order)[:capacity]
    filled = (jnp.arange(capacity, dtype=jnp.int32) < jnp.sum(member.astype(jnp.int32))).astype(jnp.float32)
    return (slot_rows, filled)

def reference(hidden, labels, targets, head_weight, cluster_weight, proj_one, proj_two, proj_three, out_one, out_two, out_three):
    groups = TOKENS // GRP_TOK
    capacity = GRP_TOK // 4
    factor = jnp.sqrt(jnp.float32(D))
    tails = ((proj_one, out_one), (proj_two, out_two), (proj_three, out_three))
    counts = jnp.stack([jnp.sum((labels == cluster).astype(jnp.float32)) for cluster in (1, 2, 3)])
    weights = TOKENS / (4.0 * counts)

    def group_terms(packed):
        rows, labs, aims = packed
        head_cap = capped(jnp.dot(rows, head_weight, preferred_element_type=jnp.float32))
        clus_cap = capped(jnp.dot(rows, cluster_weight, preferred_element_type=jnp.float32))
        head_exp = jnp.exp(head_cap)
        clus_exp = jnp.exp(clus_cap)
        total = lax.optimization_barrier(jnp.sum(head_exp, 1)) + lax.optimization_barrier(jnp.sum(clus_exp, 1))
        head_hit = ((labs == 0)[:, None] & (jnp.arange(HEAD, dtype=jnp.int32)[None, :] == aims[:, None])).astype(jnp.float32)
        clus_hit = (jnp.arange(3, dtype=jnp.int32)[None, :] + 1 == labs[:, None]).astype(jnp.float32)
        picked = lax.optimization_barrier(jnp.sum(head_hit * head_cap, 1)) + lax.optimization_barrier(jnp.sum(clus_hit * clus_cap, 1))
        token_loss = jnp.log(total) - picked
        head_grad = (factor * (head_exp / total[:, None] - head_hit) * (1.0 - (head_cap / capping) ** 2)).astype(jnp.bfloat16)
        clus_grad = factor * (clus_exp / total[:, None] - clus_hit) * (1.0 - (clus_cap / capping) ** 2)
        grads = jnp.dot(head_grad, head_weight.T, preferred_element_type=jnp.float32)
        grads = grads + jnp.dot(clus_grad, cluster_weight.astype(jnp.float32).T, precision=lax.Precision.HIGHEST)
        for number in range(3):
            proj, out = tails[number]
            slot_rows, filled = cluster_slots(labs, number + 1, capacity)
            latent = jnp.dot(rows[slot_rows], proj, preferred_element_type=jnp.float32)
            tail_cap = capped(jnp.dot(latent, out.astype(jnp.float32), precision=lax.Precision.HIGHEST))
            tail_exp = jnp.exp(tail_cap)
            tail_total = lax.optimization_barrier(jnp.sum(tail_exp, 1))
            tail_hit = (jnp.arange(out.shape[1], dtype=jnp.int32)[None, :] == aims[slot_rows][:, None]).astype(jnp.float32) * filled[:, None]
            tail_loss = (jnp.log(tail_total) - lax.optimization_barrier(jnp.sum(tail_hit * tail_cap, 1))) * filled
            tail_grad = (factor * (tail_exp / tail_total[:, None] - tail_hit) * (1.0 - (tail_cap / capping) ** 2) * filled[:, None]).astype(jnp.bfloat16)
            latent_grad = jnp.dot(tail_grad, out.T, preferred_element_type=jnp.float32)
            back = jnp.dot(latent_grad, proj.astype(jnp.float32).T, precision=lax.Precision.HIGHEST)
            token_loss = token_loss.at[slot_rows].add(weights[number] * tail_loss)
            grads = grads.at[slot_rows].add(weights[number] * back)
        return (token_loss, grads)
    losses, grads = lax.map(group_terms, (hidden.reshape(groups, GRP_TOK, D), labels.reshape(groups, GRP_TOK), targets.reshape(groups, GRP_TOK)))
    token_loss = losses.reshape(TOKENS)
    mean_loss = jnp.sum(token_loss) / TOKENS
    return (token_loss, mean_loss, grads.reshape(TOKENS, D))
```

```python
import functools

import jax
import jax.numpy as jnp
from jax import lax
from jax.experimental import pallas as pl
from jax.experimental.pallas import tpu as pltpu
from jax.sharding import PartitionSpec as P


D = 4096
capping = 30.0
bf16 = jnp.bfloat16
f32 = jnp.float32


NT = (((1,), (1,)), ((), ()))
LOG2E = 1.4426950408889634


def capped(values):
    return capping * jnp.tanh(values / capping)


def split_two(x):
    top = lax.reduce_precision(x, exponent_bits=8, mantissa_bits=7)
    return top.astype(bf16), (x - top).astype(bf16)


def split_dot(x, w, dims):
    hi, lo = split_two(x)
    return lax.dot_general(hi, w, dims, preferred_element_type=f32) + lax.dot_general(
        lo, w, dims, preferred_element_type=f32
    )


def butterfly(x, axis, size):
    step = 1
    while step < size:
        x = x + lax.ppermute(x, axis, [(i, i ^ step) for i in range(size)])
        step = step * 2
    return x


def axis_sum(x, axis):
    size = lax.axis_size(axis)
    if size & (size - 1) or size > 8:
        return lax.psum(x, axis)
    return butterfly(x, axis, size)


def line_pairs(moves):
    return [(a * 2 + b, c * 2 + b) for a, c in moves for b in range(2)]


Y_SWAP = [(a * 2 + b, a * 2 + 1 - b) for a in range(4) for b in range(2)]
INWARD = line_pairs([(0, 1), (3, 2)])
MIDDLE = line_pairs([(1, 2), (2, 1)])
OUTWARD = line_pairs([(1, 0), (2, 3)])


def hop(x, pairs):
    return lax.ppermute(x, "vocab", pairs)


def scatter_line(blocks, is_end):
    first = hop(blocks[0:3], INWARD)
    joined = blocks[0:2] + first[0:2]
    second = hop(joined, MIDDLE)
    third = hop(blocks[3] + second[0], OUTWARD)
    return jnp.where(is_end, blocks[3] + third, blocks[2] + first[2] + second[1])


def head_forward_body(gate, hidden_ref, w_ref, aim_ref, cap_ref, stat_ref, hold_ref):
    del gate
    i = pl.program_id(0)
    tokens = hidden_ref.shape[0]
    step = w_ref.shape[1]
    part = tokens // 4

    @pl.when(i == 0)
    def _():
        hold_ref[...] = jnp.zeros_like(hold_ref)

    for r in range(4):
        here = pl.ds(r * part, part)
        bent = jnp.tanh(
            jnp.dot(hidden_ref[here, :], w_ref[...], preferred_element_type=f32) * (1.0 / capping)
        )
        cap = capping * bent
        cap_ref[here, :] = cap
        hit = lax.broadcasted_iota(jnp.int32, cap.shape, 1) == aim_ref[here, :] - i * step
        grown = jnp.sum(jnp.exp(cap), 1, keepdims=True)
        pick = jnp.sum(jnp.where(hit, cap, 0.0), 1, keepdims=True)
        lane = lax.broadcasted_iota(jnp.int32, (part, 128), 1)
        hold_ref[here, :] += jnp.where(lane == 0, grown, jnp.where(lane == 1, pick, 0.0))

    @pl.when(i == pl.num_programs(0) - 1)
    def _():
        for r in range(4):
            stat_ref[:, pl.ds(r * part, part)] = hold_ref[pl.ds(r * part, part), :].T[0:8]


def head_forward(gate, hidden, weight, aim):
    tokens, features = hidden.shape
    words = weight.shape[1]
    step = min(words, 256)
    cap, stat = pl.pallas_call(
        head_forward_body,
        grid_spec=pltpu.PrefetchScalarGridSpec(
            num_scalar_prefetch=1,
            grid=(words // step,),
            in_specs=[
                pl.BlockSpec((tokens, features), lambda i, g: (0, 0)),
                pl.BlockSpec((features, step), lambda i, g: (0, i)),
                pl.BlockSpec((tokens, 1), lambda i, g: (0, 0)),
            ],
            out_specs=[
                pl.BlockSpec((tokens, step), lambda i, g: (0, i)),
                pl.BlockSpec((8, tokens), lambda i, g: (0, 0)),
            ],
            scratch_shapes=[pltpu.VMEM((tokens, 128), f32)],
        ),
        out_shape=[
            jax.ShapeDtypeStruct((tokens, words), f32),
            jax.ShapeDtypeStruct((8, tokens), f32),
        ],
        compiler_params=pltpu.CompilerParams(dimension_semantics=("arbitrary",)),
        cost_estimate=pl.CostEstimate(
            flops=2 * tokens * words * features,
            bytes_accessed=2 * features * (words + tokens) + 4 * tokens * words,
            transcendentals=2 * tokens * words,
        ),
        name="head_forward",
    )(gate, hidden, weight, aim)
    return cap, stat[0], stat[1]


def head_back_body(order, cap_ref, total_ref, aim_ref, w_ref, *rest, pieces):
    del order
    out_refs, grad_ref = rest[:-1], rest[-1]
    step = pl.program_id(0)
    half = pl.num_programs(0) // 2

    @pl.when(step == 0)
    def _():
        def strip(r, carry):
            here = pl.ds(pl.multiple_of(r * 128, 128), 128)
            cap = cap_ref[here, :].T
            hit = lax.broadcasted_iota(jnp.int32, cap.shape, 0) == aim_ref[:, here]
            scaled = jnp.exp(cap) * (1.0 / total_ref[:, here])
            slope = 1.0 - (cap * (1.0 / capping)) ** 2
            soft = jnp.where(hit, scaled - 1.0, scaled)
            grad_ref[:, here] = (float(D) ** 0.5 * soft * slope).astype(bf16)
            return carry

        lax.fori_loop(0, cap_ref.shape[0] // 128, strip, 0)

    product = jnp.dot(w_ref[...], grad_ref[...], preferred_element_type=f32)
    start = 0
    at = 0
    for kind, length in pieces:
        value = product[:, start : start + length]
        start += length
        if kind == "line":
            out_refs[at][0] = value
            at += 1
        else:

            @pl.when(step < half)
            def _(ref=out_refs[at], value=value):
                ref[0] = value

            @pl.when(step >= half)
            def _(ref=out_refs[at + 1], value=value):
                ref[0] = value

            at += 2


def head_back(order, cap, total, aim, weight, start, pieces):
    rows = sum(length for _, length in pieces)
    words = weight.shape[1]
    blocks = order.shape[0]
    half = blocks // 2
    width = weight.shape[0] // blocks
    unit = start // rows
    specs, shapes = [], []
    for kind, length in pieces:
        if kind == "line":
            specs.append(
                pl.BlockSpec((1, width, length), lambda i, o: ((i % half) * 2 + i // half, 0, 0))
            )
            shapes.append(jax.ShapeDtypeStruct((blocks, width, length), f32))
        else:
            specs.append(
                pl.BlockSpec((1, width, length), lambda i, o: (jnp.minimum(i, half - 1), 0, 0))
            )
            specs.append(
                pl.BlockSpec((1, width, length), lambda i, o: (jnp.maximum(i - half, 0), 0, 0))
            )
            shapes += [jax.ShapeDtypeStruct((half, width, length), f32)] * 2
    return pl.pallas_call(
        functools.partial(head_back_body, pieces=pieces),
        grid_spec=pltpu.PrefetchScalarGridSpec(
            num_scalar_prefetch=1,
            grid=(blocks,),
            in_specs=[
                pl.BlockSpec((rows, words), lambda i, o: (unit, 0)),
                pl.BlockSpec((1, rows), lambda i, o: (0, unit)),
                pl.BlockSpec((1, rows), lambda i, o: (0, unit)),
                pl.BlockSpec((width, words), lambda i, o: (o[i], 0)),
            ],
            out_specs=specs,
            scratch_shapes=[pltpu.VMEM((words, rows), bf16)],
        ),
        out_shape=shapes,
        compiler_params=pltpu.CompilerParams(dimension_semantics=("arbitrary",)),
        cost_estimate=pl.CostEstimate(
            flops=2 * rows * words * width * blocks,
            bytes_accessed=2 * words * width * blocks + 4 * rows * words + 4 * rows * width * blocks,
            transcendentals=rows * words,
        ),
        name="head_back",
    )(order, cap, total, aim, weight)


def gate_of(x):
    return jnp.where(x == x, 0, 1).astype(jnp.int32)


def tail_body(lat_ref, aim_ref, out_ref, acc_ref, sum_ref, hold_ref, *, slots, step, wide):
    i = pl.program_id(0)

    @pl.when(i == 0)
    def _():
        acc_ref[...] = jnp.zeros_like(acc_ref)
        hold_ref[...] = jnp.zeros_like(hold_ref)

    words = out_ref[...]
    if wide:
        both = jnp.dot(lat_ref[...], words, preferred_element_type=f32)
        scaled = both[:slots] + both[slots:]
    else:
        scaled = jnp.dot(lat_ref[...], jnp.concatenate([words, words], 0), preferred_element_type=f32)
    bent = jnp.tanh(scaled)
    grown = jnp.exp2(bent * (capping * LOG2E))
    hit = lax.broadcasted_iota(jnp.int32, bent.shape, 1) == aim_ref[...] - i * step
    hold_ref[...] += jnp.sum(grown, 1, keepdims=True)
    soft = (grown * (1.0 - bent * bent)).astype(bf16)
    hard = jnp.where(hit, 1.0, 0.0).astype(bf16)
    acc_ref[...] += lax.dot_general(
        jnp.concatenate([soft, hard], 0), words, NT, preferred_element_type=f32
    )

    @pl.when(i == pl.num_programs(0) - 1)
    def _():
        sum_ref[...] = jnp.broadcast_to(hold_ref[...], (slots, 128)).T[0:8]


def tail_pass(latent, aim, out):
    slots, width = latent.shape
    words = out.shape[1]
    step = next(s for s in (1024, 512, 256, 128) if words % s == 0)
    hi, lo = split_two(latent * (1.0 / capping))
    wide = width > 128
    pair = jnp.concatenate([hi, lo], 0 if wide else 1)
    acc, sums = pl.pallas_call(
        functools.partial(tail_body, slots=slots, step=step, wide=wide),
        grid=(words // step,),
        in_specs=[
            pl.BlockSpec(pair.shape, lambda i: (0, 0)),
            pl.BlockSpec((slots, 1), lambda i: (0, 0)),
            pl.BlockSpec((width, step), lambda i: (0, i)),
        ],
        out_specs=[
            pl.BlockSpec((2 * slots, width), lambda i: (0, 0)),
            pl.BlockSpec((8, slots), lambda i: (0, 0)),
        ],
        out_shape=[
            jax.ShapeDtypeStruct((2 * slots, width), f32),
            jax.ShapeDtypeStruct((8, slots), f32),
        ],
        scratch_shapes=[pltpu.VMEM((slots, 1), f32)],
        compiler_params=pltpu.CompilerParams(dimension_semantics=("arbitrary",)),
        cost_estimate=pl.CostEstimate(
            flops=8 * slots * words * width,
            bytes_accessed=2 * words * width + 12 * slots * width,
            transcendentals=2 * slots * words,
        ),
        name="tail_pass",
    )(pair, aim, out)
    return acc[:slots], acc[slots:], sums[0]


def per_device(
    hidden,
    labels,
    targets,
    head_weight,
    cluster_weight,
    proj_one,
    proj_two,
    proj_three,
    out_one,
    out_two,
    out_three,
):
    tokens, _ = hidden.shape
    width_local = proj_one.shape[0]
    head_local = head_weight.shape[1]
    capacity = tokens // 4
    places = lax.axis_size("vocab")
    at = lax.axis_index("vocab")
    feat_start = at * width_local
    factor = float(D) ** 0.5
    projs = (proj_one, proj_two, proj_three)
    outs = (out_one, out_two, out_three)
    own_features = lax.dynamic_slice_in_dim(hidden, feat_start, width_local, 1)

    member = labels[None, :] == jnp.arange(1, 4, dtype=jnp.int32)[:, None]
    before = jnp.arange(tokens)[:, None] <= jnp.arange(tokens)[None, :]
    placed = jnp.dot(member.astype(bf16), before.astype(bf16), preferred_element_type=f32) - 1.0
    placed = jnp.where(member, placed.astype(jnp.int32), -1)
    picked = (
        placed[:, None, :] == jnp.arange(capacity, dtype=jnp.int32)[None, :, None]
    ).reshape(3 * capacity, tokens)
    selection = picked.astype(bf16)
    slot_aims = jnp.sum(jnp.where(picked, targets[None, :], 0), 1).reshape(3, capacity)
    counts_local = jnp.sum(member.astype(f32), 1)
    filled = (jnp.arange(capacity, dtype=f32)[None, :] < counts_local[:, None]).astype(f32)
    rows = jnp.dot(selection, own_features, preferred_element_type=f32).astype(bf16)
    parts = tuple(
        jnp.dot(rows[c * capacity : (c + 1) * capacity], projs[c], preferred_element_type=f32)
        for c in range(3)
    )
    latents = lax.psum(parts, "vocab")

    local_aims = jnp.where(labels == 0, targets - at * head_local, -1)
    gate = sum(gate_of(p[0, 0]) for p in parts)
    head_cap, head_part, head_pick_part = head_forward(
        gate[None], hidden, head_weight, local_aims[:, None]
    )
    head_total = axis_sum(head_part, "vocab")
    clus_cap = capped(jnp.dot(hidden, cluster_weight, preferred_element_type=f32))
    clus_exp = jnp.exp(clus_cap)
    clus_hit = (jnp.arange(3, dtype=jnp.int32)[None, :] + 1 == labels[:, None]).astype(f32)
    total = head_total + jnp.sum(clus_exp, 1)

    total_row = total[None, :]
    aim_row = local_aims[None, :]
    if places == 8:
        line, side = at // 2, at % 2
        is_end = (line == 0) | (line == 3)
        steps = jnp.arange(4, dtype=jnp.int32)
        line_order = jnp.where(line < 2, 3 - steps, steps)
        order = jnp.concatenate([line_order * 2 + 1 - side, line_order * 2 + side])
        eighth = tokens // 8

        def back_call(gate, start, *pieces):
            return head_back(
                order + gate, head_cap, total_row, aim_row, head_weight,
                start * eighth, tuple((k, p * eighth) for k, p in pieces),
            )

        def side_first(away, mine):
            other = hop(away, Y_SWAP)
            mine = mine + other
            return scatter_line(mine, is_end)

        def line_first(blocks):
            both = scatter_line(blocks.reshape(4, 2, *blocks.shape[1:]), is_end)
            return both[1] + hop(both[0], Y_SWAP)

        piece_0, *piece_1 = back_call(0, 0, ("line", 1), ("side", 1), ("side", 2), ("side", 2))
        own = [
            line_first(piece_0),
            side_first(*piece_1[:2]),
            side_first(*piece_1[2:4]),
            side_first(*piece_1[4:]),
        ]
        gate = gate_of(piece_0[0, 0, 0])
    else:
        scaled = jnp.exp(head_cap) / total[:, None]
        slope = 1.0 - (head_cap / capping) ** 2
        head_hit = jnp.arange(head_local, dtype=jnp.int32)[None, :] == local_aims[:, None]
        head_grad = (factor * (scaled - head_hit.astype(f32)) * slope).astype(bf16)
        gate = gate_of(total[0])
        head_grads = lax.psum_scatter(
            lax.dot_general(head_grad, head_weight, NT, preferred_element_type=f32),
            "vocab",
            scatter_dimension=1,
            tiled=True,
        )

    slot_aims = jnp.where(filled > 0, slot_aims, -(2**30))
    passes = [None] * 3
    for c in (2, 0, 1):
        passes[c] = tail_pass(
            latents[c], (slot_aims[c] + gate - at * outs[c].shape[1])[:, None], outs[c]
        )
        gate = gate_of(passes[c][2][0])
    slot_picks = [capped(jnp.sum(latents[c] * passes[c][1], 1)) for c in range(3)]
    gathered = axis_sum(
        jnp.concatenate([p[2] for p in passes] + slot_picks + [head_pick_part]), "vocab"
    )
    tail_total = gathered[: 3 * capacity].reshape(3, capacity)
    tail_pick = gathered[3 * capacity : 6 * capacity].reshape(3, capacity)
    head_loss = jnp.log(total) - gathered[6 * capacity :] - jnp.sum(clus_hit * clus_cap, 1)
    tail_loss = (jnp.log(tail_total) - tail_pick) * filled
    soft_scale = factor * filled / tail_total
    hard_scale = factor * filled * (1.0 - (tail_pick / capping) ** 2)
    grad_parts = tuple(
        passes[c][0] * soft_scale[c][:, None] - passes[c][1] * hard_scale[c][:, None]
        for c in range(3)
    )
    latent_grads = lax.psum(grad_parts, "vocab")

    if places == 8:
        piece_4 = back_call(sum(gate_of(p[0, 0]) for p in grad_parts), 6, ("side", 1), ("side", 1))
        own += [side_first(*piece_4[2 * k : 2 * k + 2]) for k in range(2)]
        head_grads = jnp.concatenate(own, 1).T

    all_tokens = tokens * lax.axis_size("dp")
    dp_sums = axis_sum(
        jnp.concatenate([counts_local, jnp.sum(head_loss)[None], jnp.sum(tail_loss, 1)]), "dp"
    )
    weights = all_tokens / (4.0 * dp_sums[0:3])
    mean_loss = (dp_sums[3] + jnp.sum(weights * dp_sums[4:7])) / all_tokens
    slot_loss = (weights[:, None] * tail_loss).reshape(3 * capacity)
    token_loss = head_loss + jnp.sum(jnp.where(picked, slot_loss[:, None], 0.0), 0)

    backs = jnp.concatenate(
        [weights[c] * split_dot(latent_grads[c], projs[c], NT) for c in range(3)], 0
    )
    placed_back = split_dot_left(selection, backs)
    clus_grad = factor * (clus_exp / total[:, None] - clus_hit) * (1.0 - (clus_cap / capping) ** 2)
    clus_rows = lax.dynamic_slice_in_dim(cluster_weight, feat_start, width_local, 0).astype(f32)
    clus_back = sum(clus_grad[:, c : c + 1] * clus_rows[:, c][None, :] for c in range(3))
    return (token_loss, mean_loss, head_grads + placed_back + clus_back)


def split_dot_left(selection, x):
    hi, lo = split_two(x)
    dims = (((0,), (0,)), ((), ()))
    return lax.dot_general(selection, hi, dims, preferred_element_type=f32) + lax.dot_general(
        selection, lo, dims, preferred_element_type=f32
    )


def solution(mesh):
    return jax.shard_map(
        per_device,        mesh=mesh,
        in_specs=(
            P("dp", None),
            P("dp"),
            P("dp"),
            P(None, "vocab"),
            P(),
            P("vocab", None),
            P("vocab", None),
            P("vocab", None),
            P(None, "vocab"),
            P(None, "vocab"),
            P(None, "vocab"),
        ),
        out_specs=(P("dp"), P(), P("dp", "vocab")),
        check_vma=False,
    )
```
